512 devices in a mesh: group: 16 (over z, core), dom: 32 (over x, y).
Axes of the slice: x: 4, y: 8, z: 8, core: 2. Of those that a mesh axis runs over, the one named last changes fastest.
Arguments:
- hot_rows: bfloat16 [65536, 1024], P(('group', 'dom')), may hold values from -24 to 24
- cold_codes: bfloat16 [65536, 1024], P(('group', 'dom')), may hold values from -127 to 127
- scale_index: int32 [65536], P(('group', 'dom')), may hold values from 0 to 255
- scale_table: float32 [256], replicated, may hold values from 0.004 to 0.04
- stale_rows: bfloat16 [65536, 1024], P(('group', 'dom')), may hold values from -6 to 6
- tile_index: int32 [1024, 3], P(('group', 'dom')), may hold values from 0 to 2
- tile_count: int32 [1024], P(('group', 'dom')), may hold values from 1 to 3
- tile_values: bfloat16 [1024, 3, 128, 128], P(('group', 'dom')), may hold values from -0.3125 to 0.3125
- weight: bfloat16 [1024, 1024], P('dom'), may hold values from -0.1875 to 0.1875
- out_grad: bfloat16 [131072, 1024], P(('group', 'dom')), may hold values from -6 to 6
- stale_grads: bfloat16 [65536, 1024], P(('group', 'dom')), may hold values from -6 to 6
- send_rows: int32 [16384, 4], P(('group', 'dom')), may hold values from 0 to 255
Outputs:
- activations: bfloat16 [131072, 1024], P(('group', 'dom'))
- feature_grad: bfloat16 [131072, 1024], P(('group', 'dom'))
- weight_grad: float32 [1024, 1024], P('dom')
- next_rows: bfloat16 [65536, 1024], P(('group', 'dom'))
- next_grads: bfloat16 [65536, 1024], P(('group', 'dom'))
The draws below stay inside these ranges and needn't reach their ends.
Inputs may be any that keep to these rules, and one draw needn't show every extreme that they name: `send_rows`: rows may repeat.
All inputs are finite; a program needn't handle non-finite values.
Results may differ from the reference program's by a relative error of at most 0.0061.
Values may be sent and summed in bfloat16 or wider, within the bound.
No kernel may reach another device: no remote copies, remote signals or barrier semaphores. Data moves between devices by JAX's collectives and lax.ppermute only.
A program may use at most 64 MiB of HBM per device.

```python
import math
import jax
import jax.numpy as jnp
from jax import lax

D = 1024
CLUSTER = 128
HOT_CL = 1
COLD_CL = 1
TILES = 3
BND_ROWS = 128
NSCALE = 256
CL = 2
ROWS = 256
SRC_CL = 3
PEER_ROWS = 4
N_GROUP = 16
N_DOM = 32
DEVICES = 512


def touch_ends(drawn, own_key, smallest, high):
    spot = [jax.random.randint(jax.random.fold_in(own_key, axis), (), 0, length) for axis, length in enumerate(drawn.shape)]
    longest = drawn.shape.index(max(drawn.shape))
    neighbour = spot[:longest] + [(spot[longest] + 1) % drawn.shape[longest]] + spot[longest + 1:]
    return drawn.at[tuple(spot)].set(smallest).at[tuple(neighbour)].set(high)


def spiked(result, own_key, source, target, shards_of, factor):
    owner, partner = [(jnp.arange(result.shape[dim]) // (result.shape[dim] // shards_of)).reshape([-1 if axis == dim else 1 for axis in range(result.ndim)]) for dim in (source, target)]
    chosen = jax.random.permutation(own_key, shards_of)[partner]
    strong = (owner == chosen) | (owner == (partner + shards_of // 2) % shards_of)
    return jnp.where(strong, factor * result, result)


def steps_of(stream_key, shape, split, smallest, top_value):
    gain = 1.0
    for position, parts in split:
        heights = jax.random.uniform(jax.random.fold_in(jax.random.fold_in(stream_key, 6), position), (parts,), jnp.float32, smallest / len(split), top_value / len(split))
        gain = gain * jnp.repeat(jnp.exp(heights), shape[position] // parts).reshape((-1,) + (1,) * (len(shape) - 1 - position))
    return gain


def scatter_about(stream_key, shape, spread, reach, shards=(), held_as=jnp.bfloat16):
    array = jax.random.normal(stream_key, shape, jnp.float32) * spread
    if len(shards) > 0:
        array = steps_of(stream_key, shape, shards, -0.22, 0.18) * array
    return jnp.clip(array, min=-reach, max=reach).astype(held_as)


def bell_draw_with(key, dims, scale, reach, split, heavy, kind=jnp.bfloat16):
    entries = scale * jax.random.normal(key, dims, jnp.float32)
    if split:
        entries = entries * steps_of(key, dims, split, -0.22, 0.18)
    return jnp.clip(spiked(entries, jax.random.fold_in(key, 3), *heavy), -reach, reach).astype(kind)


def setup_inputs(seed: int = 0) -> dict:
    seeds = jax.random.split(jax.random.key(seed), 13)
    hot_rows = bell_draw_with(seeds[0], (DEVICES * HOT_CL * CLUSTER, D), 1.0, 24.0, ((0, 512),), (0, 1, 512, 6.0))
    cold_codes = jnp.clip(jax.random.uniform(seeds[1], (DEVICES * COLD_CL * CLUSTER, D), jnp.float32, -127.0, 127.0) * steps_of(seeds[1], (DEVICES * COLD_CL * CLUSTER, D), ((0, 512),), -0.4, 0.0), -127.0, 127.0).astype(jnp.bfloat16)
    scale_index = touch_ends(jax.random.randint(seeds[2], (DEVICES * COLD_CL * CLUSTER,), 0, NSCALE), jax.random.fold_in(seeds[2], 1), 0, NSCALE - 1).astype(jnp.int32)
    scale_table = jnp.clip(jnp.exp(jax.random.uniform(seeds[3], (NSCALE,), jnp.float32, math.log(0.004), math.log(0.04))), 0.004, 0.04)
    stale_rows = scatter_about(seeds[4], (DEVICES * BND_ROWS, D), 1.0, 6.0, ((0, 512),))
    tile_index = touch_ends(jax.random.randint(seeds[5], (DEVICES * CL, TILES), 0, SRC_CL), jax.random.fold_in(seeds[5], 1), 0, SRC_CL - 1).astype(jnp.int32)
    tile_count = touch_ends(jax.random.randint(seeds[6], (DEVICES * CL,), 1, TILES + 1), jax.random.fold_in(seeds[6], 1), 1, TILES).astype(jnp.int32)
    tile_values = scatter_about(seeds[7], (DEVICES * CL, TILES, CLUSTER, CLUSTER), (CLUSTER * TILES) ** -0.5, 0.3125, ((0, 512),))
    weight = scatter_about(seeds[8], (D, D), D ** -0.5, 0.1875, ((0, 32),))
    out_grad = scatter_about(seeds[9], (DEVICES * ROWS, D), 1.0, 6.0, ((0, 512),))
    stale_grads = scatter_about(seeds[10], (DEVICES * BND_ROWS, D), 1.0, 6.0, ((0, 512),))
    send_rows = touch_ends(jax.random.randint(seeds[11], (DEVICES * N_DOM, PEER_ROWS), 0, ROWS), jax.random.fold_in(seeds[11], 1), 0, ROWS - 1).astype(jnp.int32)
    return {"hot_rows": hot_rows, "cold_codes": cold_codes, "scale_index": scale_index, "scale_table": scale_table, "stale_rows": stale_rows, "tile_index": tile_index, "tile_count": tile_count, "tile_values": tile_values, "weight": weight, "out_grad": out_grad, "stale_grads": stale_grads, "send_rows": send_rows}


def dequantize(cold_codes, scale_index, scale_table):
    levels = jnp.arange(scale_table.shape[0], dtype=jnp.int32)
    lookup = jnp.sum(jnp.where(scale_index[:, None] == levels[None, :], scale_table[None, :], jnp.zeros_like(scale_table)[None, :]), axis=1)
    return (cold_codes.astype(jnp.float32) * lookup[:, None]).astype(jnp.bfloat16)


def silu_parts(preact):
    logistic = jax.nn.sigmoid(preact)
    return preact * logistic, logistic * (1.0 + preact * (1.0 - logistic))


def swap_peers(stacked):
    peer_rows = BND_ROWS // N_DOM
    blocks = stacked.reshape(N_GROUP, N_DOM, N_DOM, peer_rows, D)
    return jnp.swapaxes(blocks, 1, 2).reshape(DEVICES * BND_ROWS, D)


def reference(hot_rows, cold_codes, scale_index, scale_table, stale_rows, tile_index, tile_count, tile_values, weight, out_grad, stale_grads, send_rows):
    clusters_dev = HOT_CL + COLD_CL
    row_count = clusters_dev * CLUSTER
    src_count = clusters_dev + BND_ROWS // CLUSTER
    inputs = (hot_rows.reshape(DEVICES, HOT_CL * CLUSTER, D),
              cold_codes.reshape(DEVICES, COLD_CL * CLUSTER, D),
              scale_index.reshape(DEVICES, COLD_CL * CLUSTER),
              stale_rows.reshape(DEVICES, BND_ROWS, D),
              tile_index.reshape(DEVICES, clusters_dev, TILES),
              tile_count.reshape(DEVICES, clusters_dev),
              tile_values.reshape(DEVICES, clusters_dev, TILES, CLUSTER, CLUSTER),
              out_grad.reshape(DEVICES, row_count, D),
              stale_grads.reshape(DEVICES, BND_ROWS, D),
              send_rows.reshape(DEVICES, BND_ROWS))

    def device_step(running, pieces):
        hot, codes, indices, stale, tindex, tcount, tiles, grad_out, stale_back, sends = pieces
        local_rows = jnp.concatenate([hot, dequantize(codes, indices, scale_table)], axis=0)
        source = jnp.concatenate([local_rows, stale], axis=0).reshape(src_count, CLUSTER, D)
        live_mask = jnp.arange(TILES, dtype=jnp.int32)[None, :] < tcount[:, None]
        masked = jnp.where(live_mask[:, :, None, None], tiles, jnp.zeros_like(tiles))
        picked = jnp.take(source, tindex, axis=0)
        hidden = jnp.einsum('ckab,ckbd->cad', masked.astype(jnp.float32), picked.astype(jnp.float32))
        hidden = hidden.reshape(row_count, D).astype(jnp.bfloat16)
        preact = jnp.dot(hidden, weight, preferred_element_type=jnp.float32)
        activ, slope = silu_parts(preact)
        pre_grad = (grad_out.astype(jnp.float32) * slope).astype(jnp.bfloat16)
        partial_value = jnp.dot(hidden.T, pre_grad, preferred_element_type=jnp.float32)
        hid_grad = jnp.dot(pre_grad, weight.T, preferred_element_type=jnp.float32).astype(jnp.bfloat16)
        contrib = jnp.einsum('ckab,cad->ckbd', masked.astype(jnp.float32), hid_grad.reshape(clusters_dev, CLUSTER, D).astype(jnp.float32))
        onehot = (tindex.reshape(-1)[None, :] == jnp.arange(src_count, dtype=jnp.int32)[:, None]).astype(contrib.dtype)
        src_grad = jnp.dot(onehot, contrib.reshape(clusters_dev * TILES, CLUSTER * D), precision=lax.Precision.HIGHEST)
        src_grad = src_grad.reshape(src_count * CLUSTER, D)
        placing = (jnp.arange(row_count, dtype=jnp.int32)[:, None] == sends[None, :]).astype(jnp.bfloat16)
        returned = jnp.dot(placing, stale_back, preferred_element_type=jnp.float32)
        feature_grad = (src_grad[:row_count] + returned).astype(jnp.bfloat16)
        bound_grad = src_grad[row_count:].astype(jnp.bfloat16)
        outgoing = jnp.take(local_rows, sends, axis=0)
        return running + partial_value, (activ.astype(jnp.bfloat16), feature_grad, bound_grad, outgoing)

    start_grad = jnp.zeros((D, D), jnp.float32)
    weight_grad, stacked = lax.scan(device_step, start_grad, inputs)
    activ_all, feature_all, bound_all, outgoing_all = stacked
    activations = activ_all.reshape(DEVICES * row_count, D)
    feature_grad = feature_all.reshape(DEVICES * row_count, D)
    next_rows = swap_peers(outgoing_all)
    next_grads = swap_peers(bound_all)
    return activations, feature_grad, weight_grad, next_rows, next_grads
```

```python
import jax
import jax.numpy as jnp
from jax import lax
from jax.sharding import Mesh
from jax.sharding import PartitionSpec as P

AXES = ("z", "core", "dx", "dy")
DOM = ("dx", "dy")
SWAP = [(0, 1), (1, 0)]


def dequantize(cold_codes, scale_index, scale_table):
    levels = jnp.arange(scale_table.shape[0], dtype=jnp.int32)
    lookup = jnp.sum(
        jnp.where(scale_index[:, None] == levels[None, :], scale_table[None, :], 0.0), axis=1
    )
    return (cold_codes.astype(jnp.float32) * lookup[:, None]).astype(jnp.bfloat16)


def silu_parts(preact):
    logistic = jax.nn.sigmoid(preact)
    return (preact * logistic, logistic * (1.0 + preact * (1.0 - logistic)))


def dot(a, b, ca, cb):
    return lax.dot_general(a, b, (((ca,), (cb,)), ((), ())), preferred_element_type=jnp.float32)


def fold_index(peers, slots):
    row = jnp.arange(peers * 2 * slots, dtype=jnp.int32)
    peer, half, slot = row // (2 * slots), (row // slots) % 2, row % slots
    return peer * slots + slot, half


def unfold(folded, peers, slots):
    source, half = fold_index(peers, slots)
    flat = folded.reshape(peers * 2 * slots, -1)
    want = jnp.arange(peers * slots, dtype=jnp.int32)[:, None] == source[None, :]
    parts = [
        dot((want & (half == h)[None, :]).astype(jnp.bfloat16), flat, 1, 0).astype(jnp.bfloat16)
        for h in (0, 1)
    ]
    return jnp.concatenate(parts, axis=1)


def pick_half(both, half, width):
    return jnp.where((half == 0)[:, None], both[:, :width], both[:, width:])


def local(
    hot_rows,
    cold_codes,
    scale_index,
    scale_table,
    stale_rows,
    tile_index,
    tile_count,
    tile_values,
    weight,
    out_grad,
    stale_grads,
    send_rows,
):
    core = lax.axis_index("core")
    first = core == 0
    tile_slots = tile_values.shape[1]
    cluster_rows = tile_values.shape[2]
    peers, slots = send_rows.shape
    width = weight.shape[1]
    half_w = width // 2
    block = weight.shape[0]

    local_rows = jnp.concatenate(
        [hot_rows, dequantize(cold_codes, scale_index, scale_table)], axis=0
    )
    row_count = local_rows.shape[0]
    sends = send_rows.reshape(-1)
    slot_of, half_of = fold_index(peers, slots)
    folded_sends = jnp.broadcast_to(send_rows[:, None, :], (peers, 2, slots)).reshape(-1)
    picker = (folded_sends[:, None] == jnp.arange(row_count, dtype=jnp.int32)[None, :]).astype(
        jnp.bfloat16
    )
    outgoing = pick_half(dot(picker, local_rows, 1, 0), half_of, half_w).astype(jnp.bfloat16)
    outgoing = outgoing.reshape(peers, 2 * slots, half_w)

    my_half = jnp.where(first, weight[:, :half_w], weight[:, half_w:])
    send_w = jnp.concatenate(
        [jnp.broadcast_to(my_half[None], (peers, block, half_w)), outgoing], axis=1
    )
    got_w = lax.all_to_all(send_w, DOM, split_axis=0, concat_axis=0, tiled=True)
    w_own = got_w[:, :block].reshape(peers * block, half_w)
    next_rows = unfold(got_w[:, block:], peers, slots)
    w_oth = lax.ppermute(w_own, "core", SWAP)

    source = jnp.concatenate([local_rows, stale_rows], axis=0)
    src_count = source.shape[0] // cluster_rows
    live_mask = jnp.arange(tile_slots, dtype=jnp.int32)[None, :] < tile_count[:, None]
    masked = jnp.where(live_mask[:, :, None, None], tile_values, jnp.zeros_like(tile_values))
    selector = tile_index[:, :, None] == jnp.arange(src_count, dtype=jnp.int32)[None, None, :]
    operator = jnp.sum(
        jnp.where(
            selector[:, :, None, :, None], masked[:, :, :, None, :].astype(jnp.float32), 0.0
        ),
        axis=1,
    )
    operator = operator.reshape(row_count, src_count * cluster_rows)
    hidden = jnp.dot(operator, source.astype(jnp.float32), precision=lax.Precision.HIGHEST)
    hidden = hidden.astype(jnp.bfloat16)

    og = (out_grad[:, :half_w], out_grad[:, half_w:])
    acts, grads = [], []
    for w, flip in ((w_own, False), (w_oth, True)):
        preact = dot(hidden, w, 1, 0)
        activ, slope = silu_parts(preact)
        acts.append(activ.astype(jnp.bfloat16))
        grad = jnp.where(first != flip, og[0], og[1]).astype(jnp.float32)
        grads.append((grad * slope).astype(jnp.bfloat16))
    activations = jnp.concatenate(
        [jnp.where(first, acts[0], acts[1]), jnp.where(first, acts[1], acts[0])], axis=1
    )

    part_oth = dot(hidden, grads[1], 0, 0).astype(jnp.bfloat16)
    part_in = lax.ppermute(part_oth, "core", SWAP)
    part = (dot(hidden, grads[0], 0, 0) + part_in.astype(jnp.float32)).astype(jnp.bfloat16)

    hid_grad = dot(grads[0], w_own, 1, 1) + dot(grads[1], w_oth, 1, 1)
    hid_grad = hid_grad.astype(jnp.bfloat16)
    src_grad = lax.dot_general(
        operator,
        hid_grad.astype(jnp.float32),
        (((0,), (0,)), ((), ())),
        precision=lax.Precision.HIGHEST,
    )
    bound_grad = src_grad[row_count:].astype(jnp.bfloat16)
    folder = (
        slot_of[:, None] == jnp.arange(peers * slots, dtype=jnp.int32)[None, :]
    ).astype(jnp.bfloat16)
    back = pick_half(dot(folder, bound_grad, 1, 0), half_of, half_w).astype(jnp.bfloat16)
    send_p = jnp.concatenate(
        [part.reshape(peers, block, half_w), back.reshape(peers, 2 * slots, half_w)], axis=1
    )
    got_p = lax.all_to_all(send_p, DOM, split_axis=0, concat_axis=0, tiled=True)
    next_grads = unfold(got_p[:, block:], peers, slots)
    plane = jnp.sum(got_p[:, :block].astype(jnp.float32), axis=0).astype(jnp.bfloat16)
    planes = lax.axis_size("z")
    stack = lax.all_to_all(
        jnp.broadcast_to(plane[None], (planes, *plane.shape)), "z", 0, 0, tiled=True
    )
    total = jnp.sum(stack.astype(jnp.float32), axis=0)
    other = lax.ppermute(total, "core", SWAP)
    weight_grad = jnp.concatenate(
        [jnp.where(first, total, other), jnp.where(first, other, total)], axis=1
    )

    placing = (jnp.arange(row_count, dtype=jnp.int32)[:, None] == sends[None, :]).astype(
        jnp.bfloat16
    )
    returned = dot(placing, stale_grads, 1, 0)
    feature_grad = (src_grad[:row_count] + returned).astype(jnp.bfloat16)
    return (activations, feature_grad, weight_grad, next_rows, next_grads)


def solution(mesh):
    shape = (mesh.shape["group"] // 2, 2, 4, mesh.shape["dom"] // 4)
    torus = Mesh(mesh.devices.reshape(shape), AXES)
    rows = P(AXES, None)
    placed = (
        rows,
        rows,
        P(AXES),
        P(),
        rows,
        rows,
        P(AXES),
        P(AXES, None, None, None),
        P(DOM, None),
        rows,
        rows,
        rows,
    )
    return jax.shard_map(
        local,
        mesh=torus,
        in_specs=placed,
        out_specs=(rows, rows, P(DOM, None), rows, rows),
        check_vma=False,
    )
```

```python
import jax
import jax.numpy as jnp
from jax import lax
from jax.experimental import pallas as pl
from jax.sharding import Mesh
from jax.sharding import PartitionSpec as P


AXES = ("z", "core", "dx", "dy")
DOM = ("dx", "dy")
SWAP = [(0, 1), (1, 0)]
BF = jnp.bfloat16


def dequantize(cold_codes, scale_index, scale_table):
    levels = jnp.arange(scale_table.shape[0], dtype=jnp.int32)
    lookup = jnp.sum(
        jnp.where(scale_index[:, None] == levels[None, :], scale_table[None, :], 0.0), axis=1
    )
    return (cold_codes.astype(jnp.float32) * lookup[:, None]).astype(BF)


def silu_parts(preact):
    logistic = jax.nn.sigmoid(preact)
    return (preact * logistic, logistic * (1.0 + preact * (1.0 - logistic)))


def dot(a, b, ca, cb):
    return lax.dot_general(a, b, (((ca,), (cb,)), ((), ())), preferred_element_type=jnp.float32)


def swap_core(value):
    return lax.ppermute(value, "core", SWAP)


def halves(array, first):
    width = array.shape[1] // 2
    low, high = array[:, :width], array[:, width:]
    return jnp.where(first, low, high), jnp.where(first, high, low)


def ordered(mine, other, first):
    return jnp.concatenate(
        [jnp.where(first, mine, other), jnp.where(first, other, mine)], axis=1
    )


def core_products(hidden, hidden_peer, grad, grad_peer, w):
    rows, width = grad.shape
    depth = hidden.shape[1]

    def body(h_ref, hp_ref, g_ref, gp_ref, w_ref, act_ref, actp_ref, pre_ref, prep_ref, part_ref):
        w_all = w_ref[...]
        for h, g, a, p in (
            (h_ref, g_ref, act_ref, pre_ref),
            (hp_ref, gp_ref, actp_ref, prep_ref),
        ):
            activ, slope = silu_parts(dot(h[...], w_all, 1, 0))
            a[...] = activ.astype(BF)
            p[...] = (g[...].astype(jnp.float32) * slope).astype(BF)
        part_ref[...] = (
            dot(h_ref[...], pre_ref[...], 0, 0) + dot(hp_ref[...], prep_ref[...], 0, 0)
        ).astype(BF)

    small = jax.ShapeDtypeStruct((rows, width), BF)
    return pl.pallas_call(
        body,
        out_shape=(small, small, small, small, jax.ShapeDtypeStruct((depth, width), BF)),
        cost_estimate=pl.CostEstimate(
            flops=8 * rows * depth * width, bytes_accessed=6 * depth * width, transcendentals=0
        ),
        name="core_products",
    )(hidden, hidden_peer, grad, grad_peer, w)


def local(
    hot_rows,
    cold_codes,
    scale_index,
    scale_table,
    stale_rows,
    tile_index,
    tile_count,
    tile_values,
    weight,
    out_grad,
    stale_grads,
    send_rows,
):
    first = lax.axis_index("core") == 0
    nx, ny, nz = lax.axis_size("dx"), lax.axis_size("dy"), lax.axis_size("z")
    tile_slots = tile_values.shape[1]
    cluster_rows = tile_values.shape[2]
    slots = send_rows.shape[1]
    block = weight.shape[0]
    half_w = weight.shape[1] // 2

    def spread(value, axis, count):
        copies = jnp.broadcast_to(value[None], (count, *value.shape))
        return lax.all_to_all(copies, axis, split_axis=0, concat_axis=0, tiled=True)

    my_cols = halves(weight, first)[0]
    column = spread(my_cols, "dy", ny).reshape(ny * block, half_w)
    w = spread(column, "dx", nx).reshape(nx * ny * block, half_w)

    local_rows = jnp.concatenate(
        [hot_rows, dequantize(cold_codes, scale_index, scale_table)], axis=0
    )
    row_count = local_rows.shape[0]
    source = jnp.concatenate([local_rows, stale_rows], axis=0)
    src_count = source.shape[0] // cluster_rows
    live_mask = jnp.arange(tile_slots, dtype=jnp.int32)[None, :] < tile_count[:, None]
    masked = jnp.where(live_mask[:, :, None, None], tile_values, jnp.zeros_like(tile_values))
    selector = tile_index[:, :, None] == jnp.arange(src_count, dtype=jnp.int32)[None, None, :]
    operator = jnp.sum(
        jnp.where(
            selector[:, :, None, :, None], masked[:, :, :, None, :].astype(jnp.float32), 0.0
        ),
        axis=1,
    )
    operator = operator.reshape(row_count, src_count * cluster_rows)
    hidden = jnp.dot(operator, source.astype(jnp.float32), precision=lax.Precision.HIGHEST)
    hidden = hidden.astype(BF)
    grad_mine, grad_give = halves(out_grad, first)
    hidden_peer = swap_core(hidden)
    grad_peer = swap_core(grad_give)
    sends = send_rows.reshape(-1)
    row_ids = jnp.arange(row_count, dtype=jnp.int32)
    outgoing = dot((sends[:, None] == row_ids[None, :]).astype(BF), local_rows, 1, 0).astype(BF)

    act_mine, act_give, pre_mine, pre_peer, part = core_products(
        hidden, hidden_peer, grad_mine, grad_peer, w
    )
    got_x = lax.all_to_all(
        part.reshape(nx, ny * block, half_w), "dx", split_axis=0, concat_axis=0, tiled=True
    )

    hid_give = dot(pre_peer, w, 1, 1).astype(BF)
    hid_got = swap_core(hid_give)
    hid_grad = (dot(pre_mine, w, 1, 1) + hid_got.astype(jnp.float32)).astype(BF)
    act_got = swap_core(act_give)
    activations = ordered(act_mine, act_got, first)
    src_grad = lax.dot_general(
        operator,
        hid_grad.astype(jnp.float32),
        (((0,), (0,)), ((), ())),
        precision=lax.Precision.HIGHEST,
    )
    bound_grad = src_grad[row_count:].astype(BF)
    peers = nx * ny
    riders = jnp.concatenate(
        [outgoing.reshape(peers, slots, -1), bound_grad.reshape(peers, slots, -1)], axis=1
    )

    summed = jnp.sum(got_x.astype(jnp.float32), axis=0).astype(BF).reshape(ny, block, half_w)
    got_y = lax.all_to_all(summed, "dy", split_axis=0, concat_axis=0, tiled=True)
    total = jnp.sum(got_y.astype(jnp.float32), axis=0)
    for reach in (1, -1, 3):
        pairs = [(i, (i + (reach if i % 2 == 0 else -reach)) % nz) for i in range(nz)]
        total = total + lax.ppermute(total, "z", pairs)
    got_r = lax.all_to_all(riders, DOM, split_axis=0, concat_axis=0, tiled=True)
    next_rows = got_r[:, :slots].reshape(peers * slots, -1)
    next_grads = got_r[:, slots:].reshape(peers * slots, -1)

    weight_grad = ordered(total, swap_core(total), first)

    placing = row_ids[:, None] == sends[None, :]
    returned = dot(placing.astype(BF), stale_grads, 1, 0)
    feature_grad = (src_grad[:row_count] + returned).astype(BF)
    return (activations, feature_grad, weight_grad, next_rows, next_grads)


def solution(mesh):
    shape = (mesh.shape["group"] // 2, 2, 4, mesh.shape["dom"] // 4)
    torus = Mesh(mesh.devices.reshape(shape), AXES)
    rows = P(AXES, None)
    placed = (
        rows,
        rows,
        P(AXES),
        P(),
        rows,
        rows,
        P(AXES),
        P(AXES, None, None, None),
        P(DOM, None),
        rows,
        rows,
        rows,
    )
    return jax.shard_map(
        local,
        mesh=torus,
        in_specs=placed,
        out_specs=(rows, rows, P(DOM, None), rows, rows),
        check_vma=False,
    )
```

```python
import jax
import jax.numpy as jnp
from jax import lax
from jax.experimental import pallas as pl
from jax.experimental.pallas import tpu as pltpu
from jax.sharding import Mesh
from jax.sharding import PartitionSpec as P


AXES = ("z", "core", "dx", "dy")
DOM = ("dx", "dy")
SWAP = [(0, 1), (1, 0)]
BF = jnp.bfloat16


def dequantize(cold_codes, scale_index, scale_table):
    levels = jnp.arange(scale_table.shape[0], dtype=jnp.int32)
    lookup = jnp.sum(
        jnp.where(scale_index[:, None] == levels[None, :], scale_table[None, :], 0.0), axis=1
    )
    return (cold_codes.astype(jnp.float32) * lookup[:, None]).astype(BF)


def silu_parts(preact):
    logistic = jax.nn.sigmoid(preact)
    return (preact * logistic, logistic * (1.0 + preact * (1.0 - logistic)))


def dot(a, b, ca, cb):
    return lax.dot_general(a, b, (((ca,), (cb,)), ((), ())), preferred_element_type=jnp.float32)


def swap_core(value):
    return lax.ppermute(value, "core", SWAP)


def halves(array, first):
    width = array.shape[1] // 2
    low, high = array[:, :width], array[:, width:]
    return jnp.where(first, low, high), jnp.where(first, high, low)


def ordered(mine, other, first):
    return jnp.concatenate(
        [jnp.where(first, mine, other), jnp.where(first, other, mine)], axis=1
    )


def core_products(hidden, hidden_peer, grad, grad_peer, w):
    rows, width = grad.shape
    depth = hidden.shape[1]

    def body(h_ref, hp_ref, g_ref, gp_ref, w_ref, act_ref, actp_ref, pre_ref, prep_ref, part_ref):
        w_all = w_ref[...]
        for h, g, a, p in (
            (h_ref, g_ref, act_ref, pre_ref),
            (hp_ref, gp_ref, actp_ref, prep_ref),
        ):
            activ, slope = silu_parts(dot(h[...], w_all, 1, 0))
            a[...] = activ.astype(BF)
            p[...] = (g[...].astype(jnp.float32) * slope).astype(BF)
        part_ref[...] = (
            dot(h_ref[...], pre_ref[...], 0, 0) + dot(hp_ref[...], prep_ref[...], 0, 0)
        ).astype(BF)

    small = jax.ShapeDtypeStruct((rows, width), BF)
    return pl.pallas_call(
        body,
        out_shape=(small, small, small, small, jax.ShapeDtypeStruct((depth, width), BF)),
        cost_estimate=pl.CostEstimate(
            flops=8 * rows * depth * width, bytes_accessed=6 * depth * width, transcendentals=0
        ),
        compiler_params=pltpu.CompilerParams(vmem_limit_bytes=16 * 2**20),
        name="core_products",
    )(hidden, hidden_peer, grad, grad_peer, w)


def local(
    hot_rows,
    cold_codes,
    scale_index,
    scale_table,
    stale_rows,
    tile_index,
    tile_count,
    tile_values,
    weight,
    out_grad,
    stale_grads,
    send_rows,
):
    first = lax.axis_index("core") == 0
    nx, ny, nz = lax.axis_size("dx"), lax.axis_size("dy"), lax.axis_size("z")
    tile_slots = tile_values.shape[1]
    cluster_rows = tile_values.shape[2]
    slots = send_rows.shape[1]
    block = weight.shape[0]
    half_w = weight.shape[1] // 2

    def spread(value, axis, count):
        copies = jnp.broadcast_to(value[None], (count, *value.shape))
        return lax.all_to_all(copies, axis, split_axis=0, concat_axis=0, tiled=True)

    my_cols = lax.dynamic_slice_in_dim(weight, lax.axis_index("core") * half_w, half_w, axis=1)
    column = spread(my_cols, "dy", ny).reshape(ny * block, half_w)
    w = spread(column, "dx", nx).reshape(nx * ny * block, half_w)

    local_rows = jnp.concatenate(
        [hot_rows, dequantize(cold_codes, scale_index, scale_table)], axis=0
    )
    row_count = local_rows.shape[0]
    source = jnp.concatenate([local_rows, stale_rows], axis=0)
    src_count = source.shape[0] // cluster_rows
    live_mask = jnp.arange(tile_slots, dtype=jnp.int32)[None, :] < tile_count[:, None]
    masked = jnp.where(live_mask[:, :, None, None], tile_values, jnp.zeros_like(tile_values))
    selector = tile_index[:, :, None] == jnp.arange(src_count, dtype=jnp.int32)[None, None, :]
    operator = jnp.sum(
        jnp.where(
            selector[:, :, None, :, None], masked[:, :, :, None, :].astype(jnp.float32), 0.0
        ),
        axis=1,
    )
    operator = operator.reshape(row_count, src_count * cluster_rows)
    hidden = jnp.dot(operator, source.astype(jnp.float32), precision=lax.Precision.HIGHEST)
    hidden = hidden.astype(BF)
    grad_mine, grad_give = halves(out_grad, first)
    hidden_peer = swap_core(hidden)
    grad_peer = swap_core(grad_give)
    sends = send_rows.reshape(-1)
    row_ids = jnp.arange(row_count, dtype=jnp.int32)
    outgoing = dot((sends[:, None] == row_ids[None, :]).astype(BF), local_rows, 1, 0).astype(BF)

    act_mine, act_give, pre_mine, pre_peer, part = core_products(
        hidden, hidden_peer, grad_mine, grad_peer, w
    )
    got_x = lax.all_to_all(
        part.reshape(nx, ny * block, half_w), "dx", split_axis=0, concat_axis=0, tiled=True
    )

    hid_give = dot(pre_peer, w, 1, 1).astype(BF)
    hid_got = swap_core(hid_give)
    hid_grad = (dot(pre_mine, w, 1, 1) + hid_got.astype(jnp.float32)).astype(BF)
    act_got = swap_core(act_give)
    activations = ordered(act_mine, act_got, first)
    src_grad = lax.dot_general(
        operator,
        hid_grad.astype(jnp.float32),
        (((0,), (0,)), ((), ())),
        precision=lax.Precision.HIGHEST,
    )
    bound_grad = src_grad[row_count:].astype(BF)
    peers = nx * ny
    riders = jnp.concatenate(
        [outgoing.reshape(peers, slots, -1), bound_grad.reshape(peers, slots, -1)], axis=1
    )

    summed = jnp.sum(got_x.astype(jnp.float32), axis=0).astype(BF).reshape(ny, block, half_w)
    got_y = lax.all_to_all(summed, "dy", split_axis=0, concat_axis=0, tiled=True)
    total = jnp.sum(got_y.astype(jnp.float32), axis=0)
    stack = lax.all_gather(total.astype(BF), ("z", "core"))
    total = jnp.sum(stack.reshape(nz, 2, block, half_w).astype(jnp.float32), axis=0)
    weight_grad = jnp.concatenate([total[0], total[1]], axis=1)
    got_r = lax.all_to_all(riders, DOM, split_axis=0, concat_axis=0, tiled=True)
    flat_r = got_r.reshape(peers * 2 * slots, -1)
    slot_row = jnp.arange(peers * slots, dtype=jnp.int32)
    slot_row = slot_row + slot_row // slots * slots
    flat_ids = jnp.arange(peers * 2 * slots, dtype=jnp.int32)

    def unfold(kind):
        pick = (slot_row + kind * slots)[:, None] == flat_ids[None, :]
        return dot(pick.astype(BF), flat_r, 1, 0).astype(BF)

    next_rows, next_grads = unfold(0), unfold(1)

    placing = row_ids[:, None] == sends[None, :]
    returned = dot(placing.astype(BF), stale_grads, 1, 0)
    feature_grad = (src_grad[:row_count] + returned).astype(BF)
    return (activations, feature_grad, weight_grad, next_rows, next_grads)


def solution(mesh):
    shape = (mesh.shape["group"] // 2, 2, 4, mesh.shape["dom"] // 4)
    torus = Mesh(mesh.devices.reshape(shape), AXES)
    rows = P(AXES, None)
    placed = (
        rows,
        rows,
        P(AXES),
        P(),
        rows,
        rows,
        P(AXES),
        P(AXES, None, None, None),
        P(DOM, None),
        rows,
        rows,
        rows,
    )
    return jax.shard_map(
        local,
        mesh=torus,
        in_specs=placed,
        out_specs=(rows, rows, P(DOM, None), rows, rows),
        check_vma=False,
    )
```

```python
import jax
import jax.numpy as jnp
from jax import lax
from jax.experimental import pallas as pl
from jax.experimental.pallas import tpu as pltpu
from jax.sharding import Mesh
from jax.sharding import PartitionSpec as P


AXES = ("z", "core", "dx", "dy")
DOM = ("dx", "dy")
SWAP = [(0, 1), (1, 0)]
BF = jnp.bfloat16


def dequantize(cold_codes, scale_index, scale_table):
    levels = jnp.arange(scale_table.shape[0], dtype=jnp.int32)
    lookup = jnp.sum(
        jnp.where(scale_index[:, None] == levels[None, :], scale_table[None, :], 0.0), axis=1
    )
    return (cold_codes.astype(jnp.float32) * lookup[:, None]).astype(BF)


def silu_parts(preact):
    logistic = jax.nn.sigmoid(preact)
    return (preact * logistic, logistic * (1.0 + preact * (1.0 - logistic)))


def dot(a, b, ca, cb):
    return lax.dot_general(a, b, (((ca,), (cb,)), ((), ())), preferred_element_type=jnp.float32)


def swap_core(value):
    return lax.ppermute(value, "core", SWAP)


def halves(array, first):
    width = array.shape[1] // 2
    low, high = array[:, :width], array[:, width:]
    return jnp.where(first, low, high), jnp.where(first, high, low)


def ordered(mine, other, first):
    return jnp.concatenate(
        [jnp.where(first, mine, other), jnp.where(first, other, mine)], axis=1
    )


def kernel(body, flops, moved, mib, *shapes):
    return pl.pallas_call(
        body,
        out_shape=tuple(jax.ShapeDtypeStruct(*shape) for shape in shapes),
        cost_estimate=pl.CostEstimate(flops=flops, bytes_accessed=moved, transcendentals=0),
        compiler_params=pltpu.CompilerParams(vmem_limit_bytes=mib * 2**20),
    )


def pre_grad(h, g, w):
    activ, slope = silu_parts(dot(h, w, 1, 0))
    return activ, (g.astype(jnp.float32) * slope).astype(BF)


def weight_products(hidden, grad, peer, w):
    rows, width = grad.shape
    depth = hidden.shape[1]

    def body(h_ref, g_ref, peer_ref, w_ref, part_ref):
        w_all = w_ref[...]
        pre = pre_grad(h_ref[...], g_ref[...], w_all)[1]
        total = dot(h_ref[...], pre, 0, 0)
        pre = pre_grad(peer_ref[:, :depth], peer_ref[:, depth:], w_all)[1]
        part_ref[...] = (total + dot(peer_ref[:, :depth], pre, 0, 0)).astype(BF)

    return kernel(
        body, 8 * rows * depth * width, 6 * depth * width, 16, ((depth, width), BF)
    )(hidden, grad, peer, w)[0]


def row_products(hidden, grad, peer, w):
    rows, depth = hidden.shape
    width = w.shape[1]

    def body(h_ref, g_ref, peer_ref, w_ref, act_ref, actp_ref, hid_ref, hidp_ref):
        w_all = w_ref[...]
        activ, pre = pre_grad(peer_ref[:, :depth], peer_ref[:, depth:], w_all)
        actp_ref[...] = activ.astype(BF)
        hidp_ref[...] = dot(pre, w_all, 1, 1).astype(BF)
        activ, pre = pre_grad(h_ref[...], g_ref[...], w_all)
        act_ref[...] = activ.astype(BF)
        hid_ref[...] = dot(pre, w_all, 1, 1)

    return kernel(
        body,
        16 * rows * depth * width,
        6 * depth * width,
        16,
        ((rows, width), BF),
        ((rows, width), BF),
        ((rows, depth), jnp.float32),
        ((rows, depth), BF),
    )(hidden, grad, peer, w)


def finish(stack, riders):
    members, block, half_w = stack.shape
    peers, both, width = riders.shape
    slots = both // 2

    def body(stack_ref, riders_ref, grad_ref, rows_ref, grads_ref):
        for core in (0, 1):
            total = stack_ref[core].astype(jnp.float32)
            for plane in range(1, members // 2):
                total = total + stack_ref[2 * plane + core].astype(jnp.float32)
            grad_ref[:, core * half_w : (core + 1) * half_w] = total
        flat = riders_ref[...]
        row = lax.broadcasted_iota(jnp.int32, (peers * slots, peers * both), 0)
        place = lax.broadcasted_iota(jnp.int32, (peers * slots, peers * both), 1)
        wanted = row + lax.div(row, slots) * slots
        for kind, out in enumerate((rows_ref, grads_ref)):
            pick = jnp.where(place == wanted + kind * slots, 1.0, 0.0).astype(BF)
            out[...] = dot(pick, flat, 1, 0).astype(BF)

    return kernel(
        body,
        4 * peers * slots * peers * both * width,
        members * block * half_w * 2,
        12,
        ((block, 2 * half_w), jnp.float32),
        ((peers * slots, width), BF),
        ((peers * slots, width), BF),
    )(stack, riders.reshape(peers * both, width))


def local(
    hot_rows,
    cold_codes,
    scale_index,
    scale_table,
    stale_rows,
    tile_index,
    tile_count,
    tile_values,
    weight,
    out_grad,
    stale_grads,
    send_rows,
):
    first = lax.axis_index("core") == 0
    nx, ny = lax.axis_size("dx"), lax.axis_size("dy")
    tile_slots = tile_values.shape[1]
    cluster_rows = tile_values.shape[2]
    slots = send_rows.shape[1]
    block = weight.shape[0]
    half_w = weight.shape[1] // 2

    def spread(value, axis, count):
        copies = jnp.broadcast_to(value[None], (count, *value.shape))
        return lax.all_to_all(copies, axis, split_axis=0, concat_axis=0, tiled=True)

    copies = jnp.broadcast_to(weight[None], (ny, *weight.shape))
    copies = lax.dynamic_slice_in_dim(copies, lax.axis_index("core") * half_w, half_w, axis=2)
    column = lax.all_to_all(copies, "dy", split_axis=0, concat_axis=0, tiled=True)
    column = column.reshape(ny * block, half_w)
    w = spread(column, "dx", nx).reshape(nx * ny * block, half_w)

    local_rows = jnp.concatenate(
        [hot_rows, dequantize(cold_codes, scale_index, scale_table)], axis=0
    )
    row_count = local_rows.shape[0]
    source = jnp.concatenate([local_rows, stale_rows], axis=0)
    src_count = source.shape[0] // cluster_rows
    live_mask = jnp.arange(tile_slots, dtype=jnp.int32)[None, :] < tile_count[:, None]
    masked = jnp.where(live_mask[:, :, None, None], tile_values, jnp.zeros_like(tile_values))
    selector = tile_index[:, :, None] == jnp.arange(src_count, dtype=jnp.int32)[None, None, :]
    operator = jnp.sum(
        jnp.where(
            selector[:, :, None, :, None], masked[:, :, :, None, :].astype(jnp.float32), 0.0
        ),
        axis=1,
    )
    operator = operator.reshape(row_count, src_count * cluster_rows)
    hidden = jnp.dot(operator, source.astype(jnp.float32), precision=lax.Precision.HIGHEST)
    hidden = hidden.astype(BF)
    grad_mine, grad_give = halves(out_grad, first)
    peer = swap_core(jnp.concatenate([hidden, grad_give], axis=1))
    sends = send_rows.reshape(-1)
    row_ids = jnp.arange(row_count, dtype=jnp.int32)
    outgoing = dot((sends[:, None] == row_ids[None, :]).astype(BF), local_rows, 1, 0).astype(BF)

    part = weight_products(hidden, grad_mine, peer, w)
    got_x = lax.all_to_all(
        part.reshape(nx, ny * block, half_w), "dx", split_axis=0, concat_axis=0, tiled=True
    )

    act_mine, act_give, hid_mine, hid_give = row_products(hidden, grad_mine, peer, w)
    hid_got = swap_core(hid_give)
    hid_grad = (hid_mine + hid_got.astype(jnp.float32)).astype(BF)
    act_got = swap_core(act_give)
    activations = ordered(act_mine, act_got, first)
    src_grad = lax.dot_general(
        operator,
        hid_grad.astype(jnp.float32),
        (((0,), (0,)), ((), ())),
        precision=lax.Precision.HIGHEST,
    )
    bound_grad = src_grad[row_count:].astype(BF)
    peers = nx * ny
    riders = jnp.concatenate(
        [outgoing.reshape(peers, slots, -1), bound_grad.reshape(peers, slots, -1)], axis=1
    )

    summed = jnp.sum(got_x.astype(jnp.float32), axis=0).astype(BF).reshape(ny, block, half_w)
    got_y = lax.all_to_all(summed, "dy", split_axis=0, concat_axis=0, tiled=True)
    total = jnp.sum(got_y.astype(jnp.float32), axis=0)
    stack = lax.all_gather(total.astype(BF), ("z", "core"))
    got_r = lax.all_to_all(riders, DOM, split_axis=0, concat_axis=0, tiled=True)
    weight_grad, next_rows, next_grads = finish(stack, got_r)

    placing = row_ids[:, None] == sends[None, :]
    returned = dot(placing.astype(BF), stale_grads, 1, 0)
    feature_grad = (src_grad[:row_count] + returned).astype(BF)
    return (activations, feature_grad, weight_grad, next_rows, next_grads)


def solution(mesh):
    shape = (mesh.shape["group"] // 2, 2, 4, mesh.shape["dom"] // 4)
    torus = Mesh(mesh.devices.reshape(shape), AXES)
    rows = P(AXES, None)
    placed = (
        rows,
        rows,
        P(AXES),
        P(),
        rows,
        rows,
        P(AXES),
        P(AXES, None, None, None),
        P(DOM, None),
        rows,
        rows,
        rows,
    )
    return jax.shard_map(
        local,
        mesh=torus,
        in_specs=placed,
        out_specs=(rows, rows, P(DOM, None), rows, rows),
        check_vma=False,
    )
```

```python
import jax
import jax.numpy as jnp
from jax import lax
from jax.experimental import pallas as pl
from jax.experimental.pallas import tpu as pltpu
from jax.sharding import Mesh
from jax.sharding import PartitionSpec as P


AXES = ("z", "core", "dx", "dy")
DOM = ("dx", "dy")
SWAP = [(0, 1), (1, 0)]
BF = jnp.bfloat16


def dequantize(cold_codes, scale_index, scale_table):
    levels = jnp.arange(scale_table.shape[0], dtype=jnp.int32)
    lookup = jnp.sum(
        jnp.where(scale_index[:, None] == levels[None, :], scale_table[None, :], 0.0), axis=1
    )
    return (cold_codes.astype(jnp.float32) * lookup[:, None]).astype(BF)


def silu_parts(preact):
    logistic = jax.nn.sigmoid(preact)
    return (preact * logistic, logistic * (1.0 + preact * (1.0 - logistic)))


def dot(a, b, ca, cb):
    return lax.dot_general(a, b, (((ca,), (cb,)), ((), ())), preferred_element_type=jnp.float32)


def swap_core(value):
    return lax.ppermute(value, "core", SWAP)


def halves(array, first):
    width = array.shape[1] // 2
    low, high = array[:, :width], array[:, width:]
    return jnp.where(first, low, high), jnp.where(first, high, low)


def ordered(mine, other, first):
    return jnp.concatenate(
        [jnp.where(first, mine, other), jnp.where(first, other, mine)], axis=1
    )


def kernel(body, flops, moved, mib, *shapes):
    return pl.pallas_call(
        body,
        out_shape=tuple(jax.ShapeDtypeStruct(*shape) for shape in shapes),
        cost_estimate=pl.CostEstimate(flops=flops, bytes_accessed=moved, transcendentals=0),
        compiler_params=pltpu.CompilerParams(vmem_limit_bytes=mib * 2**20),
    )


def pre_grad(h, g, w):
    activ, slope = silu_parts(dot(h, w, 1, 0))
    return activ, (g.astype(jnp.float32) * slope).astype(BF)


def weight_products(hidden, grad, peer, w):
    rows, width = grad.shape
    depth = hidden.shape[1]

    def body(h_ref, g_ref, peer_ref, w_ref, part_ref):
        w_all = w_ref[...]
        pre = pre_grad(h_ref[...], g_ref[...], w_all)[1]
        total = dot(h_ref[...], pre, 0, 0)
        pre = pre_grad(peer_ref[:, :depth], peer_ref[:, depth:], w_all)[1]
        part_ref[...] = (total + dot(peer_ref[:, :depth], pre, 0, 0)).astype(BF)

    return kernel(
        body, 8 * rows * depth * width, 6 * depth * width, 8, ((depth, width), BF)
    )(hidden, grad, peer, w)[0]


def row_products(hidden, grad, peer, w):
    rows, depth = hidden.shape
    width = w.shape[1]

    def body(h_ref, g_ref, peer_ref, w_ref, act_ref, actp_ref, hid_ref, hidp_ref):
        w_all = w_ref[...]
        activ, pre = pre_grad(peer_ref[:, :depth], peer_ref[:, depth:], w_all)
        actp_ref[...] = activ.astype(BF)
        hidp_ref[...] = dot(pre, w_all, 1, 1).astype(BF)
        activ, pre = pre_grad(h_ref[...], g_ref[...], w_all)
        act_ref[...] = activ.astype(BF)
        hid_ref[...] = dot(pre, w_all, 1, 1)

    return kernel(
        body,
        16 * rows * depth * width,
        6 * depth * width,
        8,
        ((rows, width), BF),
        ((rows, width), BF),
        ((rows, depth), jnp.float32),
        ((rows, depth), BF),
    )(hidden, grad, peer, w)


def finish(stack, riders):
    members, block, half_w = stack.shape
    peers, both, width = riders.shape
    slots = both // 2

    def body(stack_ref, riders_ref, grad_ref, rows_ref, grads_ref):
        for core in (0, 1):
            total = stack_ref[core].astype(jnp.float32)
            for plane in range(1, members // 2):
                total = total + stack_ref[2 * plane + core].astype(jnp.float32)
            grad_ref[:, core * half_w : (core + 1) * half_w] = total
        flat = riders_ref[...]
        row = lax.broadcasted_iota(jnp.int32, (peers * slots, peers * both), 0)
        place = lax.broadcasted_iota(jnp.int32, (peers * slots, peers * both), 1)
        wanted = row + lax.div(row, slots) * slots
        for kind, out in enumerate((rows_ref, grads_ref)):
            pick = jnp.where(place == wanted + kind * slots, 1.0, 0.0).astype(BF)
            out[...] = dot(pick, flat, 1, 0).astype(BF)

    return kernel(
        body,
        4 * peers * slots * peers * both * width,
        members * block * half_w * 2,
        6,
        ((block, 2 * half_w), jnp.float32),
        ((peers * slots, width), BF),
        ((peers * slots, width), BF),
    )(stack, riders.reshape(peers * both, width))


def local(
    hot_rows,
    cold_codes,
    scale_index,
    scale_table,
    stale_rows,
    tile_index,
    tile_count,
    tile_values,
    weight,
    out_grad,
    stale_grads,
    send_rows,
):
    first = lax.axis_index("core") == 0
    nx, ny = lax.axis_size("dx"), lax.axis_size("dy")
    tile_slots = tile_values.shape[1]
    cluster_rows = tile_values.shape[2]
    slots = send_rows.shape[1]
    block = weight.shape[0]
    half_w = weight.shape[1] // 2

    def spread(value, axis, count):
        copies = jnp.broadcast_to(value[None], (count, *value.shape))
        return lax.all_to_all(copies, axis, split_axis=0, concat_axis=0, tiled=True)

    copies = jnp.broadcast_to(weight[None], (ny, *weight.shape))
    copies = lax.dynamic_slice_in_dim(copies, lax.axis_index("core") * half_w, half_w, axis=2)
    column = lax.all_to_all(copies, "dy", split_axis=0, concat_axis=0, tiled=True)
    column = column.reshape(ny * block, half_w)
    w = spread(column, "dx", nx).reshape(nx * ny * block, half_w)

    local_rows = jnp.concatenate(
        [hot_rows, dequantize(cold_codes, scale_index, scale_table)], axis=0
    )
    row_count = local_rows.shape[0]
    source = jnp.concatenate([local_rows, stale_rows], axis=0)
    src_count = source.shape[0] // cluster_rows
    live_mask = jnp.arange(tile_slots, dtype=jnp.int32)[None, :] < tile_count[:, None]
    masked = jnp.where(live_mask[:, :, None, None], tile_values, jnp.zeros_like(tile_values))
    selector = tile_index[:, :, None] == jnp.arange(src_count, dtype=jnp.int32)[None, None, :]
    operator = jnp.sum(
        jnp.where(
            selector[:, :, None, :, None], masked[:, :, :, None, :].astype(jnp.float32), 0.0
        ),
        axis=1,
    )
    operator = operator.reshape(row_count, src_count * cluster_rows)
    hidden = jnp.dot(operator, source.astype(jnp.float32), precision=lax.Precision.HIGHEST)
    hidden = hidden.astype(BF)
    grad_mine, grad_give = halves(out_grad, first)
    peer = swap_core(jnp.concatenate([hidden, grad_give], axis=1))
    sends = send_rows.reshape(-1)
    row_ids = jnp.arange(row_count, dtype=jnp.int32)
    outgoing = dot((sends[:, None] == row_ids[None, :]).astype(BF), local_rows, 1, 0).astype(BF)

    part = weight_products(hidden, grad_mine, peer, w)
    got_x = lax.all_to_all(
        part.reshape(nx, ny * block, half_w), "dx", split_axis=0, concat_axis=0, tiled=True
    )

    act_mine, act_give, hid_mine, hid_give = row_products(hidden, grad_mine, peer, w)
    hid_got = swap_core(hid_give)
    hid_grad = (hid_mine + hid_got.astype(jnp.float32)).astype(BF)
    act_got = swap_core(act_give)
    activations = ordered(act_mine, act_got, first)
    src_grad = lax.dot_general(
        operator,
        hid_grad.astype(jnp.float32),
        (((0,), (0,)), ((), ())),
        precision=lax.Precision.HIGHEST,
    )
    bound_grad = src_grad[row_count:].astype(BF)
    peers = nx * ny
    riders = jnp.concatenate(
        [outgoing.reshape(peers, slots, -1), bound_grad.reshape(peers, slots, -1)], axis=1
    )

    summed = jnp.sum(got_x.astype(jnp.float32), axis=0).astype(BF).reshape(ny, block, half_w)
    got_y = lax.all_to_all(summed, "dy", split_axis=0, concat_axis=0, tiled=True)
    total = jnp.sum(got_y.astype(jnp.float32), axis=0)
    stack = lax.all_gather(total.astype(BF), ("z", "core"))
    got_r = lax.all_to_all(riders, DOM, split_axis=0, concat_axis=0, tiled=True)
    weight_grad, next_rows, next_grads = finish(stack, got_r)

    placing = row_ids[:, None] == sends[None, :]
    returned = dot(placing.astype(BF), stale_grads, 1, 0)
    feature_grad = (src_grad[:row_count] + returned).astype(BF)
    return (activations, feature_grad, weight_grad, next_rows, next_grads)


def solution(mesh):
    shape = (mesh.shape["group"] // 2, 2, 4, mesh.shape["dom"] // 4)
    torus = Mesh(mesh.devices.reshape(shape), AXES)
    rows = P(AXES, None)
    placed = (
        rows,
        rows,
        P(AXES),
        P(),
        rows,
        rows,
        P(AXES),
        P(AXES, None, None, None),
        P(DOM, None),
        rows,
        rows,
        rows,
    )
    return jax.shard_map(
        local,
        mesh=torus,
        in_specs=placed,
        out_specs=(rows, rows, P(DOM, None), rows, rows),
        check_vma=False,
    )
```

```python
import jax
import jax.numpy as jnp
from jax import lax
from jax.experimental import pallas as pl
from jax.experimental.pallas import tpu as pltpu
from jax.sharding import Mesh
from jax.sharding import PartitionSpec as P


AXES = ("z", "core", "dx", "dy")
DOM = ("dx", "dy")
SWAP = [(0, 1), (1, 0)]
BF = jnp.bfloat16


def dequantize(cold_codes, scale_index, scale_table):
    levels = jnp.arange(scale_table.shape[0], dtype=jnp.int32)
    lookup = jnp.sum(
        jnp.where(scale_index[:, None] == levels[None, :], scale_table[None, :], 0.0), axis=1
    )
    return (cold_codes.astype(jnp.float32) * lookup[:, None]).astype(BF)


def silu_parts(preact):
    logistic = jax.nn.sigmoid(preact)
    return (preact * logistic, logistic * (1.0 + preact * (1.0 - logistic)))


def dot(a, b, ca, cb):
    return lax.dot_general(a, b, (((ca,), (cb,)), ((), ())), preferred_element_type=jnp.float32)


def swap_core(value):
    return lax.ppermute(value, "core", SWAP)


def halves(array, first):
    width = array.shape[1] // 2
    low, high = array[:, :width], array[:, width:]
    return jnp.where(first, low, high), jnp.where(first, high, low)


def ordered(mine, other, first):
    return jnp.concatenate(
        [jnp.where(first, mine, other), jnp.where(first, other, mine)], axis=1
    )


def kernel(body, flops, moved, mib, *shapes):
    return pl.pallas_call(
        body,
        out_shape=tuple(jax.ShapeDtypeStruct(*shape) for shape in shapes),
        cost_estimate=pl.CostEstimate(flops=flops, bytes_accessed=moved, transcendentals=0),
        compiler_params=pltpu.CompilerParams(vmem_limit_bytes=mib * 2**20),
    )


def pre_grad(h, g, w):
    activ, slope = silu_parts(dot(h, w, 1, 0))
    return activ, (g.astype(jnp.float32) * slope).astype(BF)


def weight_products(hidden, grad, peer, w):
    rows, width = grad.shape
    depth = hidden.shape[1]

    def body(h_ref, g_ref, peer_ref, w_ref, part_ref):
        w_all = w_ref[...]
        pre = pre_grad(h_ref[...], g_ref[...], w_all)[1]
        total = dot(h_ref[...], pre, 0, 0)
        pre = pre_grad(peer_ref[:, :depth], peer_ref[:, depth:], w_all)[1]
        part_ref[...] = (total + dot(peer_ref[:, :depth], pre, 0, 0)).astype(BF)

    return kernel(
        body, 8 * rows * depth * width, 6 * depth * width, 8, ((depth, width), BF)
    )(hidden, grad, peer, w)[0]


def row_products(hidden, grad, peer, w):
    rows, depth = hidden.shape
    width = w.shape[1]

    def body(h_ref, g_ref, peer_ref, w_ref, act_ref, hid_ref, give_ref):
        w_all = w_ref[...]
        activ, pre = pre_grad(peer_ref[:, :depth], peer_ref[:, depth:], w_all)
        give_ref[:, depth:] = activ.astype(BF)
        give_ref[:, :depth] = dot(pre, w_all, 1, 1).astype(BF)
        activ, pre = pre_grad(h_ref[...], g_ref[...], w_all)
        act_ref[...] = activ.astype(BF)
        hid_ref[...] = dot(pre, w_all, 1, 1)

    return kernel(
        body,
        16 * rows * depth * width,
        6 * depth * width,
        8,
        ((rows, width), BF),
        ((rows, depth), jnp.float32),
        ((rows, depth + width), BF),
    )(hidden, grad, peer, w)


def x_sum(terms):
    count, rows, width = terms.shape
    tile = rows // 4

    def body(terms_ref, out_ref):
        total = terms_ref[0].astype(jnp.float32)
        for i in range(1, count):
            total = total + terms_ref[i].astype(jnp.float32)
        out_ref[...] = total.astype(BF)

    return pl.pallas_call(
        body,
        grid=(4,),
        in_specs=[pl.BlockSpec((count, tile, width), lambda i: (0, i, 0))],
        out_specs=pl.BlockSpec((tile, width), lambda i: (i, 0)),
        out_shape=jax.ShapeDtypeStruct((rows, width), BF),
        compiler_params=pltpu.CompilerParams(vmem_limit_bytes=4 * 2**20),
        name="x_sum",
    )(terms)


def finish(stack, riders):
    members, block, half_w = stack.shape
    peers, both, width = riders.shape
    slots = both // 2

    def body(stack_ref, riders_ref, grad_ref, rows_ref, grads_ref):
        for core in (0, 1):
            total = stack_ref[core].astype(jnp.float32)
            for plane in range(1, members // 2):
                total = total + stack_ref[2 * plane + core].astype(jnp.float32)
            grad_ref[:, core * half_w : (core + 1) * half_w] = total
        flat = riders_ref[...]
        row = lax.broadcasted_iota(jnp.int32, (peers * slots, peers * both), 0)
        place = lax.broadcasted_iota(jnp.int32, (peers * slots, peers * both), 1)
        wanted = row + lax.div(row, slots) * slots
        for kind, out in enumerate((rows_ref, grads_ref)):
            pick = jnp.where(place == wanted + kind * slots, 1.0, 0.0).astype(BF)
            out[...] = dot(pick, flat, 1, 0).astype(BF)

    return kernel(
        body,
        4 * peers * slots * peers * both * width,
        members * block * half_w * 2,
        6,
        ((block, 2 * half_w), jnp.float32),
        ((peers * slots, width), BF),
        ((peers * slots, width), BF),
    )(stack, riders.reshape(peers * both, width))


def local(
    hot_rows,
    cold_codes,
    scale_index,
    scale_table,
    stale_rows,
    tile_index,
    tile_count,
    tile_values,
    weight,
    out_grad,
    stale_grads,
    send_rows,
):
    first = lax.axis_index("core") == 0
    nx, ny = lax.axis_size("dx"), lax.axis_size("dy")
    tile_slots = tile_values.shape[1]
    cluster_rows = tile_values.shape[2]
    slots = send_rows.shape[1]
    block = weight.shape[0]
    half_w = weight.shape[1] // 2

    def spread(value, axis, count):
        copies = jnp.broadcast_to(value[None], (count, *value.shape))
        return lax.all_to_all(copies, axis, split_axis=0, concat_axis=0, tiled=True)

    copies = jnp.broadcast_to(weight[None], (ny, *weight.shape))
    copies = lax.dynamic_slice_in_dim(copies, lax.axis_index("core") * half_w, half_w, axis=2)
    column = lax.all_to_all(copies, "dy", split_axis=0, concat_axis=0, tiled=True)
    column = column.reshape(ny * block, half_w)
    w = spread(column, "dx", nx).reshape(nx * ny * block, half_w)

    local_rows = jnp.concatenate(
        [hot_rows, dequantize(cold_codes, scale_index, scale_table)], axis=0
    )
    row_count = local_rows.shape[0]
    source = jnp.concatenate([local_rows, stale_rows], axis=0)
    src_count = source.shape[0] // cluster_rows
    live_mask = jnp.arange(tile_slots, dtype=jnp.int32)[None, :] < tile_count[:, None]
    masked = jnp.where(live_mask[:, :, None, None], tile_values, jnp.zeros_like(tile_values))
    selector = tile_index[:, :, None] == jnp.arange(src_count, dtype=jnp.int32)[None, None, :]
    operator = jnp.sum(
        jnp.where(
            selector[:, :, None, :, None], masked[:, :, :, None, :].astype(jnp.float32), 0.0
        ),
        axis=1,
    )
    operator = operator.reshape(row_count, src_count * cluster_rows)
    hidden = jnp.dot(operator, source.astype(jnp.float32), precision=lax.Precision.HIGHEST)
    hidden = hidden.astype(BF)
    grad_mine, grad_give = halves(out_grad, first)
    peer = swap_core(jnp.concatenate([hidden, grad_give], axis=1))
    sends = send_rows.reshape(-1)
    row_ids = jnp.arange(row_count, dtype=jnp.int32)
    outgoing = dot((sends[:, None] == row_ids[None, :]).astype(BF), local_rows, 1, 0).astype(BF)

    part = weight_products(hidden, grad_mine, peer, w)
    got_x = lax.all_to_all(
        part.reshape(nx, ny * block, half_w), "dx", split_axis=0, concat_axis=0, tiled=True
    )

    act_mine, hid_mine, give = row_products(hidden, grad_mine, peer, w)
    got = swap_core(give)
    depth = hidden.shape[1]
    act_got = got[:, depth:]
    hid_grad = (hid_mine + got[:, :depth].astype(jnp.float32)).astype(BF)
    activations = ordered(act_mine, act_got, first)
    src_grad = lax.dot_general(
        operator,
        hid_grad.astype(jnp.float32),
        (((0,), (0,)), ((), ())),
        precision=lax.Precision.HIGHEST,
    )
    bound_grad = src_grad[row_count:].astype(BF)
    peers = nx * ny
    riders = jnp.concatenate(
        [outgoing.reshape(peers, slots, -1), bound_grad.reshape(peers, slots, -1)], axis=1
    )

    summed = x_sum(got_x).reshape(ny, block, half_w)
    got_y = lax.all_to_all(summed, "dy", split_axis=0, concat_axis=0, tiled=True)
    total = jnp.sum(got_y.astype(jnp.float32), axis=0)
    stack = lax.all_gather(total.astype(BF), ("z", "core"))
    got_r = lax.all_to_all(riders, DOM, split_axis=0, concat_axis=0, tiled=True)
    weight_grad, next_rows, next_grads = finish(stack, got_r)

    placing = row_ids[:, None] == sends[None, :]
    returned = dot(placing.astype(BF), stale_grads, 1, 0)
    feature_grad = (src_grad[:row_count] + returned).astype(BF)
    return (activations, feature_grad, weight_grad, next_rows, next_grads)


def solution(mesh):
    shape = (mesh.shape["group"] // 2, 2, 4, mesh.shape["dom"] // 4)
    torus = Mesh(mesh.devices.reshape(shape), AXES)
    rows = P(AXES, None)
    placed = (
        rows,
        rows,
        P(AXES),
        P(),
        rows,
        rows,
        P(AXES),
        P(AXES, None, None, None),
        P(DOM, None),
        rows,
        rows,
        rows,
    )
    return jax.shard_map(
        local,
        mesh=torus,
        in_specs=placed,
        out_specs=(rows, rows, P(DOM, None), rows, rows),
        check_vma=False,
    )
```

```python
import jax
import jax.numpy as jnp
from jax import lax
from jax.experimental import pallas as pl
from jax.experimental.pallas import tpu as pltpu
from jax.sharding import Mesh
from jax.sharding import PartitionSpec as P


AXES = ("z", "core", "dx", "dy")
DOM = ("dx", "dy")
SWAP = [(0, 1), (1, 0)]
BF = jnp.bfloat16


def dequantize(cold_codes, scale_index, scale_table):
    levels = jnp.arange(scale_table.shape[0], dtype=jnp.int32)
    lookup = jnp.sum(
        jnp.where(scale_index[:, None] == levels[None, :], scale_table[None, :], 0.0), axis=1
    )
    return (cold_codes.astype(jnp.float32) * lookup[:, None]).astype(BF)


def silu_parts(preact):
    logistic = jax.nn.sigmoid(preact)
    return (preact * logistic, logistic * (1.0 + preact * (1.0 - logistic)))


def dot(a, b, ca, cb):
    return lax.dot_general(a, b, (((ca,), (cb,)), ((), ())), preferred_element_type=jnp.float32)


def swap_core(value):
    return lax.ppermute(value, "core", SWAP)


def halves(array, first):
    width = array.shape[1] // 2
    low, high = array[:, :width], array[:, width:]
    return jnp.where(first, low, high), jnp.where(first, high, low)


def ordered(mine, other, first):
    return jnp.concatenate(
        [jnp.where(first, mine, other), jnp.where(first, other, mine)], axis=1
    )


def kernel(body, flops, moved, mib, *shapes):
    return pl.pallas_call(
        body,
        out_shape=tuple(jax.ShapeDtypeStruct(*shape) for shape in shapes),
        cost_estimate=pl.CostEstimate(flops=flops, bytes_accessed=moved, transcendentals=0),
        compiler_params=pltpu.CompilerParams(vmem_limit_bytes=mib * 2**20),
    )


def pre_grad(h, g, w):
    activ, slope = silu_parts(dot(h, w, 1, 0))
    return activ, (g.astype(jnp.float32) * slope).astype(BF)


def weight_products(hidden, grad, peer, w):
    rows, width = grad.shape
    depth = hidden.shape[1]

    def body(h_ref, g_ref, peer_ref, w_ref, part_ref):
        w_all = w_ref[...]
        pre = pre_grad(h_ref[...], g_ref[...], w_all)[1]
        total = dot(h_ref[...], pre, 0, 0)
        pre = pre_grad(peer_ref[:, :depth], peer_ref[:, depth:], w_all)[1]
        part_ref[...] = (total + dot(peer_ref[:, :depth], pre, 0, 0)).astype(BF)

    return kernel(
        body, 8 * rows * depth * width, 6 * depth * width, 8, ((depth, width), BF)
    )(hidden, grad, peer, w)[0]


def row_products(hidden, grad, peer, w):
    rows, depth = hidden.shape
    width = w.shape[1]

    def body(h_ref, g_ref, peer_ref, w_ref, act_ref, hid_ref, give_ref):
        w_all = w_ref[...]
        activ, pre = pre_grad(peer_ref[:, :depth], peer_ref[:, depth:], w_all)
        give_ref[:, depth:] = activ.astype(BF)
        give_ref[:, :depth] = dot(pre, w_all, 1, 1).astype(BF)
        activ, pre = pre_grad(h_ref[...], g_ref[...], w_all)
        act_ref[...] = activ.astype(BF)
        hid_ref[...] = dot(pre, w_all, 1, 1)

    return kernel(
        body,
        16 * rows * depth * width,
        6 * depth * width,
        8,
        ((rows, width), BF),
        ((rows, depth), jnp.float32),
        ((rows, depth + width), BF),
    )(hidden, grad, peer, w)


def x_sum(terms):
    count, rows, width = terms.shape
    tile = rows // 2

    def body(terms_ref, out_ref):
        total = terms_ref[0].astype(jnp.float32)
        for i in range(1, count):
            total = total + terms_ref[i].astype(jnp.float32)
        out_ref[...] = total.astype(BF)

    return pl.pallas_call(
        body,
        grid=(2,),
        in_specs=[pl.BlockSpec((count, tile, width), lambda i: (0, i, 0))],
        out_specs=pl.BlockSpec((tile, width), lambda i: (i, 0)),
        out_shape=jax.ShapeDtypeStruct((rows, width), BF),
        compiler_params=pltpu.CompilerParams(vmem_limit_bytes=4 * 2**20),
        name="x_sum",
    )(terms)


def finish(stack, riders):
    members, block, half_w = stack.shape
    peers, both, width = riders.shape
    slots = both // 2

    def body(stack_ref, riders_ref, grad_ref, rows_ref, grads_ref):
        for core in (0, 1):
            total = stack_ref[core].astype(jnp.float32)
            for plane in range(1, members // 2):
                total = total + stack_ref[2 * plane + core].astype(jnp.float32)
            grad_ref[:, core * half_w : (core + 1) * half_w] = total
        flat = riders_ref[...]
        row = lax.broadcasted_iota(jnp.int32, (peers * slots, peers * both), 0)
        place = lax.broadcasted_iota(jnp.int32, (peers * slots, peers * both), 1)
        wanted = row + lax.div(row, slots) * slots
        for kind, out in enumerate((rows_ref, grads_ref)):
            pick = jnp.where(place == wanted + kind * slots, 1.0, 0.0).astype(BF)
            out[...] = dot(pick, flat, 1, 0).astype(BF)

    return kernel(
        body,
        4 * peers * slots * peers * both * width,
        members * block * half_w * 2,
        6,
        ((block, 2 * half_w), jnp.float32),
        ((peers * slots, width), BF),
        ((peers * slots, width), BF),
    )(stack, riders.reshape(peers * both, width))


def local(
    hot_rows,
    cold_codes,
    scale_index,
    scale_table,
    stale_rows,
    tile_index,
    tile_count,
    tile_values,
    weight,
    out_grad,
    stale_grads,
    send_rows,
):
    first = lax.axis_index("core") == 0
    nx, ny = lax.axis_size("dx"), lax.axis_size("dy")
    tile_slots = tile_values.shape[1]
    cluster_rows = tile_values.shape[2]
    slots = send_rows.shape[1]
    block = weight.shape[0]
    half_w = weight.shape[1] // 2

    def spread(value, axis, count):
        copies = jnp.broadcast_to(value[None], (count, *value.shape))
        return lax.all_to_all(copies, axis, split_axis=0, concat_axis=0, tiled=True)

    copies = jnp.broadcast_to(weight[None], (ny, *weight.shape))
    copies = lax.dynamic_slice_in_dim(copies, lax.axis_index("core") * half_w, half_w, axis=2)
    column = lax.all_to_all(copies, "dy", split_axis=0, concat_axis=0, tiled=True)
    column = column.reshape(ny * block, half_w)
    w = spread(column, "dx", nx).reshape(nx * ny * block, half_w)

    local_rows = jnp.concatenate(
        [hot_rows, dequantize(cold_codes, scale_index, scale_table)], axis=0
    )
    row_count = local_rows.shape[0]
    source = jnp.concatenate([local_rows, stale_rows], axis=0)
    src_count = source.shape[0] // cluster_rows
    live_mask = jnp.arange(tile_slots, dtype=jnp.int32)[None, :] < tile_count[:, None]
    masked = jnp.where(live_mask[:, :, None, None], tile_values, jnp.zeros_like(tile_values))
    selector = tile_index[:, :, None] == jnp.arange(src_count, dtype=jnp.int32)[None, None, :]
    operator = jnp.sum(
        jnp.where(
            selector[:, :, None, :, None], masked[:, :, :, None, :].astype(jnp.float32), 0.0
        ),
        axis=1,
    )
    operator = operator.reshape(row_count, src_count * cluster_rows)
    hidden = jnp.dot(operator, source.astype(jnp.float32), precision=lax.Precision.HIGHEST)
    hidden = hidden.astype(BF)
    grad_mine, grad_give = halves(out_grad, first)
    peer = swap_core(jnp.concatenate([hidden, grad_give], axis=1))
    sends = send_rows.reshape(-1)
    row_ids = jnp.arange(row_count, dtype=jnp.int32)
    picker = (sends[:, None] == row_ids[None, :]).astype(BF)
    outgoing = dot(picker, local_rows, 1, 0).astype(BF)

    part = weight_products(hidden, grad_mine, peer, w)
    got_x = lax.all_to_all(
        part.reshape(nx, ny * block, half_w), "dx", split_axis=0, concat_axis=0, tiled=True
    )

    act_mine, hid_mine, give = row_products(hidden, grad_mine, peer, w)
    got = swap_core(give)
    depth = hidden.shape[1]
    act_got = got[:, depth:]
    hid_grad = (hid_mine + got[:, :depth].astype(jnp.float32)).astype(BF)
    activations = ordered(act_mine, act_got, first)
    src_grad = lax.dot_general(
        operator,
        hid_grad.astype(jnp.float32),
        (((0,), (0,)), ((), ())),
        precision=lax.Precision.HIGHEST,
    )
    bound_grad = src_grad[row_count:].astype(BF)
    peers = nx * ny
    riders = jnp.concatenate(
        [outgoing.reshape(peers, slots, -1), bound_grad.reshape(peers, slots, -1)], axis=1
    )

    summed = x_sum(got_x).reshape(ny, block, half_w)
    got_y = lax.all_to_all(summed, "dy", split_axis=0, concat_axis=0, tiled=True)
    total = jnp.sum(got_y.astype(jnp.float32), axis=0)
    stack = lax.all_gather(total.astype(BF), ("z", "core"))
    got_r = lax.all_to_all(riders, DOM, split_axis=0, concat_axis=0, tiled=True)
    weight_grad, next_rows, next_grads = finish(stack, got_r)

    placing = row_ids[:, None] == sends[None, :]
    returned = dot(placing.astype(BF), stale_grads, 1, 0)
    feature_grad = (src_grad[:row_count] + returned).astype(BF)
    return (activations, feature_grad, weight_grad, next_rows, next_grads)


def solution(mesh):
    shape = (mesh.shape["group"] // 2, 2, 4, mesh.shape["dom"] // 4)
    torus = Mesh(mesh.devices.reshape(shape), AXES)
    rows = P(AXES, None)
    placed = (
        rows,
        rows,
        P(AXES),
        P(),
        rows,
        rows,
        P(AXES),
        P(AXES, None, None, None),
        P(DOM, None),
        rows,
        rows,
        rows,
    )
    return jax.shard_map(
        local,
        mesh=torus,
        in_specs=placed,
        out_specs=(rows, rows, P(DOM, None), rows, rows),
        check_vma=False,
    )
```
